32 devices in a mesh: wide: 8 (over y, x, core), narrow: 4 (over z).
Axes of the slice: x: 2, y: 2, z: 4, core: 2. Of those that a mesh axis runs over, the one named last changes fastest.
Arguments:
- panels: float32 [64, 512, 512], P('wide', 'narrow'), may hold values from -0.6 to 0.6
- factors: float32 [16, 512, 512], P('wide', 'narrow'), may hold values from -2 to 2
- member: int32 [16, 4], replicated, may hold values from 0 to 63, as said below
- target: int32 [16, 10], replicated, may hold values from 0 to 7
- ancestors: float32 [8, 512, 512], P('wide', 'narrow'), may hold values from -6 to 6
Outputs:
- updated: float32 [8, 512, 512], P('wide', 'narrow')
The draws below stay inside these ranges and needn't reach their ends.
Inputs may be any that keep to these rules, and one draw needn't show every extreme that they name: `member`: the blocks of supernode s are 4 distinct indices in [(s // 2) * 8, (s // 2 + 1) * 8); every block belongs to exactly one supernode.
All inputs are finite; a program needn't handle non-finite values.
Results may differ from the reference program's by a relative error of at most 0.0003.
Values sent between devices are 32-bit elements; how exact they have to be, the bound alone decides.
A program may use at most 128 MiB of HBM per device.

```python
import math
import jax
import jax.numpy as jnp
import numpy as np
from jax import lax

W = 512
NB = 4
SUP_DEV = 2
NP = 10
SUPER = 16
BLOCKS = 64
ANC = 8


def draw_factors(key, part):
    diag_key = jax.random.fold_in(key, 11)
    off_key = jax.random.fold_in(key, 12)
    diagonal = jax.random.uniform(diag_key, (SUPER, W), jnp.float32, 0.5, 2.0)
    offdiag = jnp.clip(jax.random.normal(off_key, (SUPER, W, W), jnp.float32), -6.0, 6.0) * (0.5 / jnp.sqrt(jnp.float32(W)))
    eye = jnp.eye(W, dtype=jnp.float32)
    return offdiag * (1.0 - eye)[None] + diagonal[:, :, None] * eye[None]


def draw_member(key, part):
    owners = SUPER // SUP_DEV
    keys = jax.random.split(jax.random.fold_in(key, 21), owners)
    shuffled = jax.vmap(lambda single: jax.random.permutation(single, SUP_DEV * NB))(keys)
    offsets = jnp.arange(owners, dtype=jnp.int32)[:, None] * (SUP_DEV * NB)
    return (shuffled.astype(jnp.int32) + offsets).reshape(SUPER, NB)


def with_ends(drawn, key, smallest, high):
    spot = [jax.random.randint(jax.random.fold_in(key, axis), (), 0, length) for axis, length in enumerate(drawn.shape)]
    longest = drawn.shape.index(max(drawn.shape))
    next_to = spot[:longest] + [(spot[longest] + 1) % drawn.shape[longest]] + spot[longest + 1:]
    return drawn.at[tuple(spot)].set(smallest).at[tuple(next_to)].set(high)


def steps_of(key, extent, cuts, low, top_value):
    level, own = 1.0, jax.random.fold_in(key, 6)
    for dim, parts in cuts:
        draws = jnp.exp(jax.random.uniform(jax.random.fold_in(own, dim), (parts,), jnp.float32, low / len(cuts), top_value / len(cuts)))
        level = level * jnp.repeat(draws, extent[dim] // parts).reshape([-1 if axis == dim else 1 for axis in range(len(extent))])
    return level


def rank_table(number_of, slope):
    loads = [(1 << 20) // math.isqrt(rank ** slope) + 1 for rank in range(1, number_of + 1)]
    spread = 1 + sum(loads) // (1 << 30)
    return np.cumsum(np.array([max(1, weight // spread) for weight in loads]))


def ranked_ids(stream_key, extent, number_of, skew):
    grid = rank_table(number_of, skew)
    lot = jax.random.randint(jax.random.fold_in(stream_key, 1), extent, 0, int(grid[number_of - 1]))
    standing = jnp.searchsorted(jnp.asarray(grid, jnp.int32), lot, side="right")
    return jax.random.permutation(jax.random.fold_in(stream_key, 2), number_of)[standing].astype(jnp.int32)


def gaussian(key, shape, width, most, cuts=(), kind=jnp.bfloat16):
    level = steps_of(key, shape, cuts, -0.22, 0.18) if cuts else 1.0
    values = jax.random.normal(key, shape, jnp.float32) * width * level
    return jnp.minimum(jnp.maximum(values, -most), most).astype(kind)


def setup_inputs(seed: int = 0) -> dict:
    splits = jax.random.split(jax.random.key(seed), 6)
    panels = gaussian(splits[0], (BLOCKS, W, W), 0.1, 0.6, ((0, 8), (1, 4)), jnp.float32)
    factors = draw_factors(jax.random.fold_in(splits[5], 71), 0)
    member = draw_member(jax.random.fold_in(splits[5], 71), 0)
    target = with_ends(ranked_ids(splits[3], (SUPER, NP), ANC, 2), jax.random.fold_in(splits[3], 3), 0, ANC - 1).astype(jnp.int32)
    ancestors = gaussian(splits[4], (ANC, W, W), 1.0, 6.0, ((0, 8), (1, 4)), jnp.float32)
    return {"panels": panels, "factors": factors, "member": member, "target": target, "ancestors": ancestors}


def pair_lists(count):
    left_pick = []
    right_pick = []
    for upper in range(count):
        for lower in range(upper + 1):
            left_pick.append(upper)
            right_pick.append(lower)
    return np.array(left_pick, dtype=np.int32), np.array(right_pick, dtype=np.int32)


def reference(panels, factors, member, target, ancestors):
    left_pick, right_pick = pair_lists(member.shape[1])
    highest = lax.Precision.HIGHEST

    def advance(running, inputs):
        members, factor, targets = inputs
        blocks = panels[members]
        scaled = jnp.einsum("kij,jm->kim", blocks, factor, precision=highest)
        updates = jnp.einsum("pim,pjm->pij", scaled[left_pick], scaled[right_pick], precision=highest)
        onehot = (targets[:, None] == jnp.arange(ANC, dtype=jnp.int32)[None, :]).astype(jnp.float32)
        return running + jnp.einsum("pa,pij->aij", onehot, updates, precision=highest), None

    running, ignored = lax.scan(advance, jnp.zeros((ANC, W, W), jnp.float32), (member, factors, target))
    return ancestors - running
```

```python
import functools

import jax
import jax.numpy as jnp
from jax import lax
from jax.experimental import pallas as pl
from jax.experimental.pallas import tpu as pltpu
from jax.sharding import PartitionSpec as P

MESH = pl.DeviceIdType.MESH
CORES = 2
ROWS_DOT = (((1,), (1,)), ((), ()))
COLS_DOT = (((1,), (0,)), ((), ()))


def halves(x):
    hi = x.astype(jnp.bfloat16)
    return hi, (x - hi.astype(jnp.float32)).astype(jnp.bfloat16)


def dot3(ah, al, bh, bl, dims):
    dot = functools.partial(
        lax.dot_general, dimension_numbers=dims, preferred_element_type=jnp.float32
    )
    return dot(ah, bh) + (dot(ah, bl) + dot(al, bh))


def kernel(cfg, weight, blocks, factors, ancestors, out, p_recv, f_full, fh, fl, s_full, s_hi, s_lo,
           upd, portion, xy_recv, zsum, z_recv, loc_sem, fs_sem, fr_sem, f2s_sem, f2r_sem, ps_sem, pr_sem,
           ss_sem, sr_sem, xs_sem, xr_sem, zs_sem, zr_sem):
    n, q_count, sups, nb, width, part, unit, split = cfg
    wide = lax.axis_index("wide")
    z = lax.axis_index("narrow")
    core = lax.rem(wide, CORES)
    q = lax.div(wide, CORES)
    mine = lax.rem(z, unit) * CORES + core
    my_unit = lax.div(z, unit)
    src_core = lax.div(my_unit, sups)

    def at(q_, core_, z_):
        return {"wide": q_ * CORES + core_, "narrow": z_}

    barrier = pltpu.get_barrier_semaphore()
    for i in range(1, CORES * n):
        other = lax.rem(z * CORES + core + i, CORES * n)
        pl.semaphore_signal(barrier, inc=1, device_id=at(q, lax.rem(other, CORES), lax.div(other, CORES)),
                            device_id_type=MESH)
    for i in range(1, q_count):
        pl.semaphore_signal(barrier, inc=1, device_id=at(lax.rem(q + i, q_count), core, z), device_id_type=MESH)
    pl.semaphore_wait(barrier, CORES * n - 1 + q_count - 1)

    anc_copy = pltpu.make_async_copy(ancestors.at[0], out.at[0], loc_sem)
    anc_copy.start()

    def remote(src, dst, send, recv, dev):
        return pltpu.make_async_remote_copy(src_ref=src, dst_ref=dst, send_sem=send, recv_sem=recv,
                                            device_id=dev, device_id_type=MESH)

    def source_copies(what, i):
        s, e = i // split, i % split
        chip = (core * sups + s) * unit + e // CORES
        to_self = jnp.logical_and(chip == z, core == e % CORES)
        rows = pl.ds(e * part, part)
        if what == "f":
            src, dst, ssem, rsem = factors.at[s, rows], f_full.at[z, e], fs_sem.at[i], fr_sem.at[z]
        else:
            src, dst, ssem, rsem = blocks.at[s, :, rows], p_recv.at[z], ps_sem.at[i], pr_sem.at[z]
        return to_self, pltpu.make_async_copy(src, dst, rsem), remote(src, dst, ssem, rsem, at(q, e % CORES, chip))

    for what in ("f", "p"):
        for i in range(sups * split):
            to_self, local, away = source_copies(what, i)
            pl.when(to_self)(local.start)
            pl.when(jnp.logical_not(to_self))(away.start)

    def arrived(ref, sem):
        pltpu.make_async_copy(ref, ref, sem).wait()

    for i in range(n):
        arrived(f_full.at[i, mine], fr_sem.at[i])

    def peer(i):
        other = lax.rem(mine + i, split)
        return other, at(q, lax.rem(other, CORES), my_unit * unit + lax.div(other, CORES))

    f_copies = []
    for i in range(1, split):
        other, dev = peer(i)
        f_copies.append(remote(f_full.at[:, mine], f_full.at[:, mine], f2s_sem.at[other], f2r_sem.at[mine], dev))
        f_copies[-1].start()
    for i in range(1, split):
        other, dev = peer(i)
        arrived(f_full.at[:, other], f2r_sem.at[other])
    hi, lo = halves(f_full[...].reshape(width, width))
    fh[...] = hi
    fl[...] = lo

    def scale(i, carry):
        zz = lax.rem(z + i, n)
        arrived(p_recv.at[zz], pr_sem.at[zz])
        ph, plo = halves(p_recv[zz].reshape(nb * part, width))
        s = dot3(ph, plo, fh[...], fl[...], COLS_DOT).reshape(nb, part, width)
        s_full[:, zz, mine] = s
        for j in range(1, split):
            other, dev = peer(j)
            remote(s_full.at[:, zz, mine], s_full.at[:, zz, mine], ss_sem.at[zz, other],
                   sr_sem.at[zz, mine], dev).start()
        sh, sl = halves(s)
        s_hi[:, zz, mine] = sh
        s_lo[:, zz, mine] = sl
        return carry

    lax.fori_loop(0, n, scale, 0)

    def take(i, carry):
        zz = lax.rem(z + i, n)
        for j in range(1, split):
            other, dev = peer(j)
            arrived(s_full.at[:, zz, other], sr_sem.at[zz, other])
            sh, sl = halves(s_full[:, zz, other])
            s_hi[:, zz, other] = sh
            s_lo[:, zz, other] = sl
        return carry

    lax.fori_loop(0, n, take, 0)

    for k in range(nb):
        def update(l, carry, k=k):
            u = dot3(s_hi[k, :, mine].reshape(n * part, width), s_lo[k, :, mine].reshape(n * part, width),
                     s_hi[l].reshape(width, width), s_lo[l].reshape(width, width), ROWS_DOT)
            upd[k * (k + 1) // 2 + l] = u.reshape(n, part, width)
            return carry

        lax.fori_loop(0, k + 1, update, 0)

    pairs = nb * (nb + 1) // 2
    step = 8

    def group(i):
        return lax.rem(z + n // 2 + i, n)

    def xy_copy(zz, other):
        pair = pl.ds(other * CORES, CORES)
        return remote(portion.at[pair, zz], xy_recv.at[q, :, zz], xs_sem.at[other, zz], xr_sem.at[q, zz],
                      at(other, core, z))

    def tiles(i, carry):
        zz = group(lax.div(i, q_count))
        other = lax.rem(q + 1 + lax.rem(i, q_count), q_count)

        def rows(r, inner):
            at_rows = pl.ds(pl.multiple_of(r * step, step), step)
            parts = [upd[p, zz, at_rows] for p in range(pairs)]
            for c in range(CORES):
                tile = other * CORES + c
                portion[tile, zz, at_rows] = sum(weight[tile, p] * parts[p] for p in range(pairs))
            return inner

        lax.fori_loop(0, part // step, rows, 0)

        @pl.when(other != q)
        def _():
            xy_copy(zz, other).start()

        return carry

    lax.fori_loop(0, n * q_count, tiles, 0)

    def z_copy(zz, c):
        return remote(zsum.at[zz, c], z_recv.at[z, core], zs_sem.at[zz, c], zr_sem.at[z, core], at(q, c, zz))

    def gather(i, carry):
        zz = group(i)
        for j in range(1, q_count):
            other = lax.rem(q + j, q_count)
            arrived(xy_recv.at[other, :, zz], xr_sem.at[other, zz])
        total = portion[pl.ds(q * CORES, CORES), zz]
        for j in range(1, q_count):
            total = total + xy_recv[lax.rem(q + j, q_count), :, zz]
        zsum[zz] = total
        for c in range(CORES):
            own = jnp.logical_and(zz == z, core == c)

            @pl.when(own)
            def _():
                z_recv[z, core] = total[c]

            @pl.when(jnp.logical_not(own))
            def _():
                z_copy(zz, c).start()

        return carry

    lax.fori_loop(0, n, gather, 0)

    for i in range(1, CORES * n):
        other = lax.rem(z * CORES + core + i, CORES * n)
        oz, oc = lax.div(other, CORES), lax.rem(other, CORES)
        arrived(z_recv.at[oz, oc], zr_sem.at[oz, oc])
    anc_copy.wait()
    for e in range(split):
        rows = pl.ds(e * part, part)
        out[0, rows] = out[0, rows] - sum(z_recv[u * unit + e // CORES, e % CORES] for u in range(n // unit))

    for what in ("f", "p"):
        for i in range(sups * split):
            to_self, local, away = source_copies(what, i)
            pl.when(jnp.logical_not(to_self))(away.wait_send)
    for copy in f_copies:
        copy.wait_send()

    def sent(i, carry):
        for j in range(1, split):
            other, dev = peer(j)
            remote(s_full.at[:, i, mine], s_full.at[:, i, mine], ss_sem.at[i, other],
                   sr_sem.at[i, mine], dev).wait_send()
        for j in range(1, q_count):
            xy_copy(i, lax.rem(q + j, q_count)).wait_send()
        for c in range(CORES):
            @pl.when(jnp.logical_not(jnp.logical_and(i == z, core == c)))
            def _():
                z_copy(i, c).wait_send()
        return carry

    lax.fori_loop(0, n, sent, 0)


def shards(panels, factors, member, target, ancestors):
    sups, blk_count, nb = factors.shape[0], panels.shape[0], member.shape[1]
    width = panels.shape[2]
    n, wide_count = lax.axis_size("narrow"), lax.axis_size("wide")
    q_count = wide_count // CORES
    tile_count = ancestors.shape[0] * wide_count
    assert ancestors.shape[0] == 1 and n % (CORES * sups) == 0
    unit = n // (CORES * sups)
    split = unit * CORES
    part = panels.shape[1] // split
    wide, z = lax.axis_index("wide"), lax.axis_index("narrow")
    own_members = lax.dynamic_slice_in_dim(member, wide * sups, sups, 0) - wide * blk_count
    blocks = panels[own_members]
    supernode = (wide // CORES) * (CORES * sups) + z // unit
    own_targets = lax.dynamic_slice_in_dim(target, supernode, 1, 0)
    weight = (own_targets == jnp.arange(tile_count, dtype=jnp.int32)[:, None]).astype(jnp.float32)
    pairs = target.shape[1]
    f32, bf16 = jnp.float32, jnp.bfloat16
    dma = pltpu.SemaphoreType.DMA
    cfg = (n, q_count, sups, nb, width, part, unit, split)
    any_space = pl.BlockSpec(memory_space=pl.ANY)
    return pl.pallas_call(
        functools.partial(kernel, cfg),
        out_shape=jax.ShapeDtypeStruct(ancestors.shape, f32),
        in_specs=[pl.BlockSpec(memory_space=pltpu.SMEM), any_space, any_space, any_space],
        out_specs=pl.BlockSpec(memory_space=pltpu.VMEM),
        scratch_shapes=[
            pltpu.VMEM((n, nb, part, width), f32),
            pltpu.VMEM((n, split, part, width), f32),
            pltpu.VMEM((width, width), bf16),
            pltpu.VMEM((width, width), bf16),
            pltpu.VMEM((nb, n, split, part, width), f32),
            pltpu.VMEM((nb, n, split, part, width), bf16),
            pltpu.VMEM((nb, n, split, part, width), bf16),
            pltpu.VMEM((pairs, n, part, width), f32),
            pltpu.VMEM((tile_count, n, part, width), f32),
            pltpu.VMEM((q_count, CORES, n, part, width), f32),
            pltpu.VMEM((n, CORES, part, width), f32),
            pltpu.VMEM((n, CORES, part, width), f32),
            dma,
            dma((sups * split,)), dma((n,)),
            dma((split,)), dma((split,)),
            dma((sups * split,)), dma((n,)),
            dma((n, split)), dma((n, split)),
            dma((q_count, n)), dma((q_count, n)),
            dma((n, CORES)), dma((n, CORES)),
        ],
        compiler_params=pltpu.CompilerParams(
            collective_id=0, has_side_effects=True, vmem_limit_bytes=58 * 2**20
        ),
        name="level",
    )(weight, blocks, factors, ancestors)


def solution(mesh):
    return jax.shard_map(
        shards,
        mesh=mesh,
        in_specs=(
            P("wide", "narrow", None),
            P("wide", "narrow", None),
            P(),
            P(),
            P("wide", "narrow", None),
        ),
        out_specs=P("wide", "narrow", None),
        check_vma=False,
    )
```

```python
import functools

import jax
import jax.numpy as jnp
from jax import lax
from jax.experimental import pallas as pl
from jax.experimental.pallas import tpu as pltpu
from jax.sharding import PartitionSpec as P

MESH = pl.DeviceIdType.MESH
CORES = 2
ROWS_DOT = (((1,), (1,)), ((), ()))
COLS_DOT = (((1,), (0,)), ((), ()))


def halves(x):
    hi = x.astype(jnp.bfloat16)
    return hi, (x - hi.astype(jnp.float32)).astype(jnp.bfloat16)


def dot3(ah, al, bh, bl, dims):
    dot = functools.partial(
        lax.dot_general, dimension_numbers=dims, preferred_element_type=jnp.float32
    )
    return dot(ah, bh) + (dot(ah, bl) + dot(al, bh))


def kernel(cfg, weight, blocks, factors, ancestors, out, p_recv, f_full, fh, fl, s_full, s_hi, s_lo,
           upd, portion, xy_recv, zsum, z_recv, loc_sem, fs_sem, fr_sem, f2s_sem, f2r_sem, ps_sem, pr_sem,
           ss_sem, sr_sem, xs_sem, xr_sem, zs_sem, zr_sem, turn_sem):
    n, q_count, sups, nb, width, part, unit, split = cfg
    units = CORES * sups
    mid = units // 2
    rows_own = unit * part
    cols = width // units
    wide = lax.axis_index("wide")
    z = lax.axis_index("narrow")
    core = lax.rem(wide, CORES)
    q = lax.div(wide, CORES)
    mine = lax.rem(z, unit) * CORES + core
    my_unit = lax.div(z, unit)
    half = lax.div(my_unit, mid)
    far_sender = core != half

    def at(q_, core_, z_):
        return {"wide": q_ * CORES + core_, "narrow": z_}

    def order(i):
        h, j = i // mid, i % mid
        near = half * mid + lax.rem(my_unit - half * mid + j, mid)
        far = mid + j - half * (1 + 2 * j)
        return (1 - h) * near + h * far

    barrier = pltpu.get_barrier_semaphore()
    for i in range(1, CORES * n):
        other = lax.rem(z * CORES + core + i, CORES * n)
        pl.semaphore_signal(barrier, inc=1, device_id=at(q, lax.rem(other, CORES), lax.div(other, CORES)),
                            device_id_type=MESH)
    for i in range(1, q_count):
        pl.semaphore_signal(barrier, inc=1, device_id=at(lax.rem(q + i, q_count), core, z), device_id_type=MESH)
    pl.semaphore_wait(barrier, CORES * n - 1 + q_count - 1)

    anc_copy = pltpu.make_async_copy(ancestors.at[0], out.at[0], loc_sem)
    anc_copy.start()

    def remote(src, dst, send, recv, dev):
        return pltpu.make_async_remote_copy(src_ref=src, dst_ref=dst, send_sem=send, recv_sem=recv,
                                            device_id=dev, device_id_type=MESH)

    def source_copy(what, i, local):
        s, e = i // split, i % split
        chip = (core * sups + s) * unit + e // CORES
        rows = pl.ds(e * part, part)
        if what == "f":
            src, dst, ssem, rsem = factors.at[s, rows], f_full.at[z, e], fs_sem.at[i], fr_sem.at[z]
        else:
            src, dst, ssem, rsem = blocks.at[s, :, rows], p_recv.at[z], ps_sem.at[i], pr_sem.at[z]
        if local:
            return pltpu.make_async_copy(src, dst, rsem)
        return remote(src, dst, ssem, rsem, at(q, e % CORES, chip))

    def to_self(i):
        s, e = i // split, i % split
        return jnp.logical_and((core * sups + s) * unit + e // CORES == z, core == e % CORES)

    def send_all(what):
        for i in range(sups * split):
            @pl.when(to_self(i))
            def _():
                source_copy(what, i, True).start()

            @pl.when(jnp.logical_not(to_self(i)))
            def _():
                source_copy(what, i, False).start()

    inner = jnp.logical_or(my_unit == mid - 1, my_unit == mid)
    outer_unit = half * (units - 1)
    outer_far = jnp.logical_and(far_sender, my_unit == outer_unit)
    inner_far = jnp.logical_and(far_sender, inner)
    send_all("f")
    pl.when(jnp.logical_not(outer_far))(lambda: send_all("p"))

    def arrived(ref, sem):
        pltpu.make_async_copy(ref, ref, sem).wait()

    for i in range(n):
        arrived(f_full.at[i, mine], fr_sem.at[i])

    def peer(i):
        other = lax.rem(mine + i, split)
        return other, at(q, lax.rem(other, CORES), my_unit * unit + lax.div(other, CORES))

    f_copies = []
    for i in range(1, split):
        other, dev = peer(i)
        f_copies.append(remote(f_full.at[:, mine], f_full.at[:, mine], f2s_sem.at[other], f2r_sem.at[mine], dev))
        f_copies[-1].start()
    for i in range(1, split):
        other, dev = peer(i)
        arrived(f_full.at[:, other], f2r_sem.at[other])
    hi, lo = halves(f_full[...].reshape(width, width))
    fh[...] = hi
    fl[...] = lo

    def s_copy(zz, j):
        other, dev = peer(j)
        return remote(s_full.at[:, zz, mine], s_full.at[:, zz, mine], ss_sem.at[zz, other],
                      sr_sem.at[zz, mine], dev)

    def scale(a):
        for m in range(unit):
            zz = a * unit + m
            arrived(p_recv.at[zz], pr_sem.at[zz])
            ph, plo = halves(p_recv[zz].reshape(nb * part, width))
            s = dot3(ph, plo, fh[...], fl[...], COLS_DOT).reshape(nb, part, width)
            s_full[:, zz, mine] = s
            for j in range(1, split):
                s_copy(zz, j).start()
            sh, sl = halves(s)
            s_hi[:, zz, mine] = sh
            s_lo[:, zz, mine] = sl
        for m in range(unit):
            zz = a * unit + m
            for j in range(1, split):
                other, dev = peer(j)
                arrived(s_full.at[:, zz, other], sr_sem.at[zz, other])
                sh, sl = halves(s_full[:, zz, other])
                s_hi[:, zz, other] = sh
                s_lo[:, zz, other] = sl

    def xy_copy(a, b, other):
        return remote(portion.at[a, b, pl.ds(other * CORES, CORES)], xy_recv.at[q, a, b],
                      xs_sem.at[other, a, b], xr_sem.at[q, a, b], at(other, core, z))

    lefts = nb // 2

    def block(a, b):
        az, bz = pl.ds(a * unit, unit), pl.ds(b * unit, unit)
        for first in range(0, nb, lefts):
            ks, ls = pl.ds(first, nb - first), pl.ds(first, lefts)
            left = [r[ks, az, mine].reshape((nb - first) * rows_own, width) for r in (s_hi, s_lo)]
            right = [r[ls, bz].reshape(lefts * cols, width) for r in (s_hi, s_lo)]
            upd[first * rows_own:, first * cols:(first + lefts) * cols] = dot3(*left, *right, ROWS_DOT)

        def tiles(i, carry):
            other = lax.rem(q + 1 + i, q_count)
            sums = [None] * CORES
            p = 0
            for k in range(nb):
                for l in range(k + 1):
                    u = upd[k * rows_own:(k + 1) * rows_own, l * cols:(l + 1) * cols]
                    for c in range(CORES):
                        term = weight[other * CORES + c, p] * u
                        sums[c] = term if p == 0 else sums[c] + term
                    p += 1
            for c in range(CORES):
                portion[a, b, other * CORES + c] = sums[c]

            @pl.when(other != q)
            def _():
                xy_copy(a, b, other).start()

            return carry

        lax.fori_loop(0, q_count, tiles, 0)

    for i in range(units):
        if i == mid:
            @pl.when(inner_far)
            def _():
                for j in range(sups * split):
                    source_copy("p", j, False).wait_send()
                pl.semaphore_signal(turn_sem, inc=1, device_id=at(q, core, z - unit + 2 * unit * half),
                                    device_id_type=MESH)

            @pl.when(outer_far)
            def _():
                pl.semaphore_wait(turn_sem, 1)
                send_all("p")

        new = order(i)
        scale(new)

        def blocks_of(j, carry, i=i, new=new):
            old = jnp.minimum(j, i)
            row = order(old)
            block(row, order(jnp.where(j < i, i, j - i)))
            return carry

        lax.fori_loop(0, 2 * i + 1, blocks_of, 0)

    def z_copy(zz, c):
        return remote(zsum.at[zz, c], z_recv.at[z, core], zs_sem.at[zz, c], zr_sem.at[z, core], at(q, c, zz))

    def gather(i, carry):
        a = order(i)
        for b in range(units):
            total = portion[a, b, pl.ds(q * CORES, CORES)]
            for j in range(1, q_count):
                other = lax.rem(q + j, q_count)
                arrived(xy_recv.at[other, a, b], xr_sem.at[other, a, b])
                total = total + xy_recv[other, a, b]
            for m in range(unit):
                zsum[a * unit + m, :, :, b * cols:(b + 1) * cols] = total[:, m * part:(m + 1) * part]
        for m in range(unit):
            zz = a * unit + m
            for c in range(CORES):
                own = jnp.logical_and(zz == z, core == c)

                @pl.when(own)
                def _():
                    z_recv[z, core] = zsum[zz, c]

                @pl.when(jnp.logical_not(own))
                def _():
                    z_copy(zz, c).start()

        return carry

    lax.fori_loop(0, units, gather, 0)

    for i in range(1, CORES * n):
        other = lax.rem(z * CORES + core + i, CORES * n)
        oz, oc = lax.div(other, CORES), lax.rem(other, CORES)
        arrived(z_recv.at[oz, oc], zr_sem.at[oz, oc])
    anc_copy.wait()
    for e in range(split):
        rows = pl.ds(e * part, part)
        out[0, rows] = out[0, rows] - sum(z_recv[u * unit + e // CORES, e % CORES] for u in range(n // unit))

    for i in range(sups * split):
        @pl.when(jnp.logical_not(to_self(i)))
        def _():
            source_copy("f", i, False).wait_send()

        @pl.when(jnp.logical_not(jnp.logical_or(to_self(i), inner_far)))
        def _():
            source_copy("p", i, False).wait_send()
    for copy in f_copies:
        copy.wait_send()

    def sent(i, carry):
        for j in range(1, split):
            s_copy(i, j).wait_send()
        for c in range(CORES):
            @pl.when(jnp.logical_not(jnp.logical_and(i == z, core == c)))
            def _():
                z_copy(i, c).wait_send()
        return carry

    lax.fori_loop(0, n, sent, 0)

    def sent_xy(i, carry):
        for j in range(1, q_count):
            xy_copy(i // units, i % units, lax.rem(q + j, q_count)).wait_send()
        return carry

    lax.fori_loop(0, units * units, sent_xy, 0)


def shards(panels, factors, member, target, ancestors):
    sups, blk_count, nb = factors.shape[0], panels.shape[0], member.shape[1]
    width = panels.shape[2]
    n, wide_count = lax.axis_size("narrow"), lax.axis_size("wide")
    q_count = wide_count // CORES
    tile_count = ancestors.shape[0] * wide_count
    assert ancestors.shape[0] == 1 and n % (CORES * sups) == 0 and CORES == 2 and nb % 2 == 0 and sups == 2
    unit = n // (CORES * sups)
    split = unit * CORES
    part = panels.shape[1] // split
    wide, z = lax.axis_index("wide"), lax.axis_index("narrow")
    own_members = lax.dynamic_slice_in_dim(member, wide * sups, sups, 0) - wide * blk_count
    blocks = panels[own_members]
    supernode = (wide // CORES) * (CORES * sups) + z // unit
    own_targets = lax.dynamic_slice_in_dim(target, supernode, 1, 0)
    weight = (own_targets == jnp.arange(tile_count, dtype=jnp.int32)[:, None]).astype(jnp.float32)
    units = CORES * sups
    cols = width // units
    f32, bf16 = jnp.float32, jnp.bfloat16
    dma = pltpu.SemaphoreType.DMA
    cfg = (n, q_count, sups, nb, width, part, unit, split)
    any_space = pl.BlockSpec(memory_space=pl.ANY)
    return pl.pallas_call(
        functools.partial(kernel, cfg),
        out_shape=jax.ShapeDtypeStruct(ancestors.shape, f32),
        in_specs=[pl.BlockSpec(memory_space=pltpu.SMEM), any_space, any_space, any_space],
        out_specs=pl.BlockSpec(memory_space=pltpu.VMEM),
        scratch_shapes=[
            pltpu.VMEM((n, nb, part, width), f32),
            pltpu.VMEM((n, split, part, width), f32),
            pltpu.VMEM((width, width), bf16),
            pltpu.VMEM((width, width), bf16),
            pltpu.VMEM((nb, n, split, part, width), f32),
            pltpu.VMEM((nb, n, split, part, width), bf16),
            pltpu.VMEM((nb, n, split, part, width), bf16),
            pltpu.VMEM((nb * unit * part, nb * cols), f32),
            pltpu.VMEM((units, units, tile_count, unit * part, cols), f32),
            pltpu.VMEM((q_count, units, units, CORES, unit * part, cols), f32),
            pltpu.VMEM((n, CORES, part, width), f32),
            pltpu.VMEM((n, CORES, part, width), f32),
            dma,
            dma((sups * split,)), dma((n,)),
            dma((split,)), dma((split,)),
            dma((sups * split,)), dma((n,)),
            dma((n, split)), dma((n, split)),
            dma((q_count, units, units)), dma((q_count, units, units)),
            dma((n, CORES)), dma((n, CORES)),
            pltpu.SemaphoreType.REGULAR,
        ],
        compiler_params=pltpu.CompilerParams(
            collective_id=0, has_side_effects=True, vmem_limit_bytes=58 * 2**20
        ),
        name="level",
    )(weight, blocks, factors, ancestors)


def solution(mesh):
    return jax.shard_map(
        shards,
        mesh=mesh,
        in_specs=(
            P("wide", "narrow", None),
            P("wide", "narrow", None),
            P(),
            P(),
            P("wide", "narrow", None),
        ),
        out_specs=P("wide", "narrow", None),
        check_vma=False,
    )
```

```python
import functools

import jax
import jax.numpy as jnp
from jax import lax
from jax.experimental import pallas as pl
from jax.experimental.pallas import tpu as pltpu
from jax.sharding import PartitionSpec as P

MESH = pl.DeviceIdType.MESH
CORES = 2
ROWS_DOT = (((1,), (1,)), ((), ()))
COLS_DOT = (((1,), (0,)), ((), ()))


def halves(x):
    hi = x.astype(jnp.bfloat16)
    return hi, (x - hi.astype(jnp.float32)).astype(jnp.bfloat16)


def dot3(ah, al, bh, bl, dims):
    dot = functools.partial(
        lax.dot_general, dimension_numbers=dims, preferred_element_type=jnp.float32
    )
    return dot(ah, bh) + (dot(ah, bl) + dot(al, bh))


def kernel(cfg, member, target, panels, factors, ancestors, out, weight, held, blocks, p_recv, f_full, fh, fl, s_full, s_hi, s_lo,
           upd, portion, xy_recv, zsum, z_recv, loc_sem, fs_sem, fr_sem, f2s_sem, f2r_sem, ps_sem, pr_sem,
           ss_sem, sr_sem, xs_sem, xr_sem, zs_sem, zr_sem, turn_sem, held_sem):
    n, q_count, sups, nb, width, part, unit, split = cfg
    units = CORES * sups
    mid = units // 2
    rows_own = unit * part
    cols = width // units
    wide = lax.axis_index("wide")
    z = lax.axis_index("narrow")
    core = lax.rem(wide, CORES)
    q = lax.div(wide, CORES)
    mine = lax.rem(z, unit) * CORES + core
    my_unit = lax.div(z, unit)
    half = lax.div(my_unit, mid)
    far_sender = core != half

    def at(q_, core_, z_):
        return {"wide": q_ * CORES + core_, "narrow": z_}

    def order(i):
        h, j = i // mid, i % mid
        near = half * mid + lax.rem(my_unit - half * mid + j, mid)
        far = mid + j - half * (1 + 2 * j)
        return (1 - h) * near + h * far

    held_copy = pltpu.make_async_copy(panels, held, held_sem)
    held_copy.start()

    barrier = pltpu.get_barrier_semaphore()
    for i in range(1, CORES * n):
        other = lax.rem(z * CORES + core + i, CORES * n)
        pl.semaphore_signal(barrier, inc=1, device_id=at(q, lax.rem(other, CORES), lax.div(other, CORES)),
                            device_id_type=MESH)
    for i in range(1, q_count):
        pl.semaphore_signal(barrier, inc=1, device_id=at(lax.rem(q + i, q_count), core, z), device_id_type=MESH)
    pl.semaphore_wait(barrier, CORES * n - 1 + q_count - 1)

    anc_copy = pltpu.make_async_copy(ancestors.at[0], out.at[0], loc_sem)
    anc_copy.start()

    def remote(src, dst, send, recv, dev):
        return pltpu.make_async_remote_copy(src_ref=src, dst_ref=dst, send_sem=send, recv_sem=recv,
                                            device_id=dev, device_id_type=MESH)

    def source_copy(what, i, local):
        s, e = i // split, i % split
        chip = (core * sups + s) * unit + e // CORES
        rows = pl.ds(e * part, part)
        if what == "f":
            src, dst, ssem, rsem = factors.at[s, rows], f_full.at[z, e], fs_sem.at[i], fr_sem.at[z]
        else:
            src, dst, ssem, rsem = blocks.at[s, :, rows], p_recv.at[z], ps_sem.at[i], pr_sem.at[z]
        if local:
            return pltpu.make_async_copy(src, dst, rsem)
        return remote(src, dst, ssem, rsem, at(q, e % CORES, chip))

    def to_self(i):
        s, e = i // split, i % split
        return jnp.logical_and((core * sups + s) * unit + e // CORES == z, core == e % CORES)

    def send_all(what):
        for i in range(sups * split):
            @pl.when(to_self(i))
            def _():
                source_copy(what, i, True).start()

            @pl.when(jnp.logical_not(to_self(i)))
            def _():
                source_copy(what, i, False).start()

    inner = jnp.logical_or(my_unit == mid - 1, my_unit == mid)
    outer_unit = half * (units - 1)
    outer_far = jnp.logical_and(far_sender, my_unit == outer_unit)
    inner_far = jnp.logical_and(far_sender, inner)
    send_all("f")
    held_copy.wait()

    def pick(i, carry):
        s, k = i // nb, i % nb
        blocks[s, k] = held[lax.rem(member[wide * sups + s, k], sups * nb)]
        return carry

    lax.fori_loop(0, sups * nb, pick, 0)
    pl.when(jnp.logical_not(outer_far))(lambda: send_all("p"))

    supernode = q * units + my_unit

    def weigh(tile, carry):
        for p in range(nb * (nb + 1) // 2):
            weight[tile, p] = jnp.where(target[supernode, p] == tile, jnp.float32(1), jnp.float32(0))
        return carry

    lax.fori_loop(0, q_count * CORES, weigh, 0)

    def arrived(ref, sem):
        pltpu.make_async_copy(ref, ref, sem).wait()

    for i in range(n):
        arrived(f_full.at[i, mine], fr_sem.at[i])

    def peer(i):
        other = lax.rem(mine + i, split)
        return other, at(q, lax.rem(other, CORES), my_unit * unit + lax.div(other, CORES))

    f_copies = []
    for i in range(1, split):
        other, dev = peer(i)
        f_copies.append(remote(f_full.at[:, mine], f_full.at[:, mine], f2s_sem.at[other], f2r_sem.at[mine], dev))
        f_copies[-1].start()
    for i in range(1, split):
        other, dev = peer(i)
        arrived(f_full.at[:, other], f2r_sem.at[other])
    hi, lo = halves(f_full[...].reshape(width, width))
    fh[...] = hi
    fl[...] = lo

    def s_copy(zz, j):
        other, dev = peer(j)
        return remote(s_full.at[:, zz, mine], s_full.at[:, zz, mine], ss_sem.at[zz, other],
                      sr_sem.at[zz, mine], dev)

    def scale(a):
        for m in range(unit):
            zz = a * unit + m
            arrived(p_recv.at[zz], pr_sem.at[zz])
            ph, plo = halves(p_recv[zz].reshape(nb * part, width))
            s = dot3(ph, plo, fh[...], fl[...], COLS_DOT).reshape(nb, part, width)
            s_full[:, zz, mine] = s
            for j in range(1, split):
                s_copy(zz, j).start()
            sh, sl = halves(s)
            s_hi[:, zz, mine] = sh
            s_lo[:, zz, mine] = sl
        for m in range(unit):
            zz = a * unit + m
            for j in range(1, split):
                other, dev = peer(j)
                arrived(s_full.at[:, zz, other], sr_sem.at[zz, other])
                sh, sl = halves(s_full[:, zz, other])
                s_hi[:, zz, other] = sh
                s_lo[:, zz, other] = sl

    def xy_copy(a, b, other):
        return remote(portion.at[a, b, pl.ds(other * CORES, CORES)], xy_recv.at[q, a, b],
                      xs_sem.at[other, a, b], xr_sem.at[q, a, b], at(other, core, z))

    lefts = nb // 2

    def block(a, b):
        az, bz = pl.ds(a * unit, unit), pl.ds(b * unit, unit)
        for first in range(0, nb, lefts):
            ks, ls = pl.ds(first, nb - first), pl.ds(first, lefts)
            left = [r[ks, az, mine].reshape((nb - first) * rows_own, width) for r in (s_hi, s_lo)]
            right = [r[ls, bz].reshape(lefts * cols, width) for r in (s_hi, s_lo)]
            upd[first * rows_own:, first * cols:(first + lefts) * cols] = dot3(*left, *right, ROWS_DOT)

        def tiles(i, carry):
            other = lax.rem(q + 1 + i, q_count)
            sums = [None] * CORES
            p = 0
            for k in range(nb):
                for l in range(k + 1):
                    u = upd[k * rows_own:(k + 1) * rows_own, l * cols:(l + 1) * cols]
                    for c in range(CORES):
                        term = weight[other * CORES + c, p] * u
                        sums[c] = term if p == 0 else sums[c] + term
                    p += 1
            for c in range(CORES):
                portion[a, b, other * CORES + c] = sums[c]

            @pl.when(other != q)
            def _():
                xy_copy(a, b, other).start()

            return carry

        lax.fori_loop(0, q_count, tiles, 0)

    for i in range(units):
        if i == mid:
            @pl.when(inner_far)
            def _():
                for j in range(sups * split - 1):
                    source_copy("p", j, False).wait_send()
                pl.semaphore_signal(turn_sem, inc=1, device_id=at(q, core, z - unit + 2 * unit * half),
                                    device_id_type=MESH)

            @pl.when(outer_far)
            def _():
                pl.semaphore_wait(turn_sem, 1)
                send_all("p")

        new = order(i)
        scale(new)

        def blocks_of(j, carry, i=i, new=new):
            ahead = i - mid if i == units - 1 else i
            rest = j - ahead - (i + 1)
            old = mid + j if i == units - 1 else j
            row = jnp.where(j < ahead, old, jnp.where(rest < 0, i, mid - 1 - rest))
            col = jnp.where(jnp.logical_and(j >= ahead, rest < 0), j - ahead, i)
            block(order(row), order(col))
            return carry

        lax.fori_loop(0, 2 * i + 1, blocks_of, 0)

    def z_copy(zz, c):
        return remote(zsum.at[zz, c], z_recv.at[z, core], zs_sem.at[zz, c], zr_sem.at[z, core], at(q, c, zz))

    def gather(i, carry):
        a = order(jnp.where(i < mid, mid + i, units - 1 - i))
        for b in range(units):
            total = portion[a, b, pl.ds(q * CORES, CORES)]
            for j in range(1, q_count):
                other = lax.rem(q + j, q_count)
                arrived(xy_recv.at[other, a, b], xr_sem.at[other, a, b])
                total = total + xy_recv[other, a, b]
            for m in range(unit):
                zsum[a * unit + m, :, :, b * cols:(b + 1) * cols] = total[:, m * part:(m + 1) * part]
        for m in range(unit):
            zz = a * unit + m
            for c in range(CORES):
                own = jnp.logical_and(zz == z, core == c)

                @pl.when(own)
                def _():
                    z_recv[z, core] = zsum[zz, c]

                @pl.when(jnp.logical_not(own))
                def _():
                    z_copy(zz, c).start()

        return carry

    lax.fori_loop(0, units, gather, 0)

    for i in range(1, CORES * n):
        other = lax.rem(z * CORES + core + i, CORES * n)
        oz, oc = lax.div(other, CORES), lax.rem(other, CORES)
        arrived(z_recv.at[oz, oc], zr_sem.at[oz, oc])
    anc_copy.wait()
    for e in range(split):
        rows = pl.ds(e * part, part)
        out[0, rows] = out[0, rows] - sum(z_recv[u * unit + e // CORES, e % CORES] for u in range(n // unit))

    for i in range(sups * split):
        @pl.when(jnp.logical_not(to_self(i)))
        def _():
            source_copy("f", i, False).wait_send()

        done = jnp.logical_or(to_self(i), inner_far) if i < sups * split - 1 else to_self(i)

        @pl.when(jnp.logical_not(done))
        def _():
            source_copy("p", i, False).wait_send()
    for copy in f_copies:
        copy.wait_send()

    def sent(i, carry):
        for j in range(1, split):
            s_copy(i, j).wait_send()
        for c in range(CORES):
            @pl.when(jnp.logical_not(jnp.logical_and(i == z, core == c)))
            def _():
                z_copy(i, c).wait_send()
        return carry

    lax.fori_loop(0, n, sent, 0)

    def sent_xy(i, carry):
        for j in range(1, q_count):
            xy_copy(i // units, i % units, lax.rem(q + j, q_count)).wait_send()
        return carry

    lax.fori_loop(0, units * units, sent_xy, 0)


def shards(panels, factors, member, target, ancestors):
    sups, nb = factors.shape[0], member.shape[1]
    width = panels.shape[2]
    n, wide_count = lax.axis_size("narrow"), lax.axis_size("wide")
    q_count = wide_count // CORES
    tile_count = ancestors.shape[0] * wide_count
    assert ancestors.shape[0] == 1 and n % (CORES * sups) == 0 and CORES == 2 and nb % 2 == 0 and sups == 2
    assert panels.shape[0] == sups * nb
    unit = n // (CORES * sups)
    split = unit * CORES
    part = panels.shape[1] // split
    units = CORES * sups
    cols = width // units
    f32, bf16 = jnp.float32, jnp.bfloat16
    dma = pltpu.SemaphoreType.DMA
    cfg = (n, q_count, sups, nb, width, part, unit, split)
    any_space = pl.BlockSpec(memory_space=pl.ANY)
    return pl.pallas_call(
        functools.partial(kernel, cfg),
        out_shape=jax.ShapeDtypeStruct(ancestors.shape, f32),
        in_specs=[pl.BlockSpec(memory_space=pltpu.SMEM)] * 2 + [any_space] * 3,
        out_specs=pl.BlockSpec(memory_space=pltpu.VMEM),
        scratch_shapes=[
            pltpu.SMEM((tile_count, target.shape[1]), f32),
            pltpu.VMEM(panels.shape, f32),
            pltpu.VMEM((sups, nb) + panels.shape[1:], f32),
            pltpu.VMEM((n, nb, part, width), f32),
            pltpu.VMEM((n, split, part, width), f32),
            pltpu.VMEM((width, width), bf16),
            pltpu.VMEM((width, width), bf16),
            pltpu.VMEM((nb, n, split, part, width), f32),
            pltpu.VMEM((nb, n, split, part, width), bf16),
            pltpu.VMEM((nb, n, split, part, width), bf16),
            pltpu.VMEM((nb * unit * part, nb * cols), f32),
            pltpu.VMEM((units, units, tile_count, unit * part, cols), f32),
            pltpu.VMEM((q_count, units, units, CORES, unit * part, cols), f32),
            pltpu.VMEM((n, CORES, part, width), f32),
            pltpu.VMEM((n, CORES, part, width), f32),
            dma,
            dma((sups * split,)), dma((n,)),
            dma((split,)), dma((split,)),
            dma((sups * split,)), dma((n,)),
            dma((n, split)), dma((n, split)),
            dma((q_count, units, units)), dma((q_count, units, units)),
            dma((n, CORES)), dma((n, CORES)),
            pltpu.SemaphoreType.REGULAR,
            dma,
        ],
        compiler_params=pltpu.CompilerParams(
            collective_id=0, has_side_effects=True, vmem_limit_bytes=58 * 2**20
        ),
        name="level",
    )(member, target, panels, factors, ancestors)


def solution(mesh):
    return jax.shard_map(
        shards,
        mesh=mesh,
        in_specs=(
            P("wide", "narrow", None),
            P("wide", "narrow", None),
            P(),
            P(),
            P("wide", "narrow", None),
        ),
        out_specs=P("wide", "narrow", None),
        check_vma=False,
    )
```
